32 devices in a mesh: blk: 16 (over z, y, core), aux: 2 (over x).
Axes of the slice: x: 2, y: 2, z: 4, core: 2. Of those that a mesh axis runs over, the one named last changes fastest.
Arguments:
- panels: bfloat16 [4, 11264, 120, 120], P(None, ('blk', 'aux')), may hold values from -0.19921875 to 0.19921875
- aux_counts: int32 [32], replicated, may hold values from 1 to 352, 9000 in all
- pair_list: int32 [64, 2], replicated, may hold values from 0 to 3
- pair_ranks: int32 [64], replicated, may hold values from 24 to 120
- amplitudes: bfloat16 [64, 120, 120], P('blk'), may hold values from -6 to 6
Outputs:
- residual: float32 [64, 120, 120], P('blk', 'aux')
The draws below stay inside these ranges and needn't reach their ends.
Inputs may be any that keep to these rules, and one draw needn't show every extreme that they name: `aux_counts`: entry k counts the live auxiliary functions of panel shard k (slots k * 352 onward), which come first in the shard; the entries sum to 9000.
All inputs are finite; a program needn't handle non-finite values.
Results may differ from the reference program's by a relative error of at most 0.0029.
Values may be sent and summed in bfloat16 or wider, within the bound.
A program may use at most 128 MiB of HBM per device.

```python
import math
import jax
import jax.numpy as jnp
import numpy as np
from jax import lax

R = 120
NAUX = 9000
NOCC = 4
PAIRS_DEV = 4
AUX_SLOT = 352
AUX_ROWS = 11264
PAIRS = 64
N_BLK = 16
N_AUX = 2
DEVICES = 32


def with_ends(values, key, smallest, largest):
    longest = values.shape.index(max(values.shape))
    spots = []
    for shift in (0, 1):
        where = [jax.random.randint(jax.random.fold_in(key, axis), (), 0, length) for axis, length in enumerate(values.shape)]
        where[longest] = (where[longest] + shift) % values.shape[longest]
        spots.append(tuple(where))
    return values.at[spots[0]].set(smallest).at[spots[1]].set(largest)


def block_scale(key, extent, shards, least, high):
    factor_of = 1.0
    for position, shards_of in shards:
        heights = jax.random.uniform(jax.random.fold_in(jax.random.fold_in(key, 6), position), (shards_of,), jnp.float32, least / len(shards), high / len(shards))
        factor_of = factor_of * jnp.repeat(jnp.exp(heights), extent[position] // shards_of).reshape((-1,) + (1,) * (len(extent) - 1 - position))
    return factor_of


def profile(count, total, bound, lean):
    weights = [(1 << 20) // math.isqrt(rank ** lean) + 1 for rank in range(2, count + 1)]
    surplus, given = total - bound - (count - 1), [1] * (count - 1)
    while surplus > 0:
        movable = [i for i in range(count - 1) if given[i] < bound]
        mass, remaining = sum([weights[i] for i in movable]), surplus
        for i in movable:
            addition = min(bound - given[i], max(1, remaining * weights[i] // mass), surplus)
            given[i] = given[i] + addition
            surplus = surplus - addition
    return np.array([bound] + given)


def ragged_sizes(stream_key, amount, total, bound, slope):
    if amount == 2:
        one = jax.random.randint(stream_key, (), max(1, total - bound), min(bound, total - 1) + 1)
        return jnp.stack([one, total - one])
    sizes = jnp.asarray(profile(amount, total, bound, slope), jnp.int32)
    twos = (amount - 1) // 2
    source_of, receiver = sizes[1:1 + 2 * twos:2], sizes[2:2 + 2 * twos:2]
    room = jnp.minimum(source_of - 1, bound - receiver)
    shifted = jax.random.randint(jax.random.fold_in(stream_key, 1), (twos,), 0, 1 << 20) % (room + 1)
    sizes = sizes.at[1:1 + 2 * twos:2].set(source_of - shifted).at[2:2 + 2 * twos:2].set(receiver + shifted)
    return sizes[jax.random.permutation(jax.random.fold_in(stream_key, 2), amount)]


def noise(own_key, dims, spread, reach, split=(), kind=jnp.bfloat16):
    loudness = block_scale(own_key, dims, split, -0.22, 0.18) if split else 1.0
    array = jax.random.normal(own_key, dims, jnp.float32) * spread * loudness
    return jnp.minimum(jnp.maximum(array, -reach), reach).astype(kind)


def setup_inputs(seed: int = 0) -> dict:
    key_of = jax.random.split(jax.random.key(seed), 6)
    panels = noise(key_of[0], (NOCC, AUX_ROWS, R, R), 0.03, 0.19921875, ((1, 32),))
    aux_counts = ragged_sizes(key_of[1], DEVICES, NAUX, AUX_SLOT, 1).astype(jnp.int32)
    pair_list = with_ends(jax.random.randint(key_of[2], (PAIRS, 2), 0, NOCC), jax.random.fold_in(key_of[2], 1), 0, NOCC - 1).astype(jnp.int32)
    pair_ranks = with_ends(jax.random.randint(key_of[3], (PAIRS,), R // 5, R + 1), jax.random.fold_in(key_of[3], 1), R // 5, R).astype(jnp.int32)
    amplitudes = noise(key_of[4], (PAIRS, R, R), 1.0, 6.0, ((0, 16),))
    return dict(panels=panels, aux_counts=aux_counts, pair_list=pair_list, pair_ranks=pair_ranks, amplitudes=amplitudes)


pair_group = 4


def ladder(block, count, pair_rows, rank_rows, amp_rows):
    slot_count = block.shape[1]
    pno_width = block.shape[2]
    live_slots = jnp.arange(slot_count, dtype=jnp.int32) < count
    positions = jnp.arange(pno_width, dtype=jnp.int32)
    group_count = pair_rows.shape[0] // pair_group

    def one_group(group_item):
        group_pairs, group_ranks, group_amps = group_item
        kept_mask = positions[None, :] < group_ranks[:, None]
        pair_mask = kept_mask[:, :, None] & kept_mask[:, None, :]
        masked = jnp.where(pair_mask, group_amps, jnp.zeros_like(group_amps))
        left_panel = jnp.take(block, group_pairs[:, 0], axis=0)
        right_panel = jnp.take(block, group_pairs[:, 1], axis=0)
        half_step = jnp.einsum("gsac,gcd->gsad", left_panel.astype(jnp.float32), masked.astype(jnp.float32))
        half_step = jnp.where(live_slots[None, :, None, None], half_step, jnp.zeros_like(half_step)).astype(jnp.bfloat16)
        ladder_sum = jnp.einsum("gsad,gsbd->gab", half_step.astype(jnp.float32), right_panel.astype(jnp.float32))
        return jnp.where(pair_mask, ladder_sum, jnp.zeros_like(ladder_sum))

    results = lax.map(one_group, (pair_rows.reshape(group_count, pair_group, 2), rank_rows.reshape(group_count, pair_group), amp_rows.reshape(group_count, pair_group, pno_width, pno_width)))
    return results.reshape(pair_rows.shape[0], pno_width, pno_width)


def reference(panels, aux_counts, pair_list, pair_ranks, amplitudes):
    blocked = panels.reshape(NOCC, N_BLK, N_AUX, AUX_SLOT, R, R)
    counts_grid = aux_counts.reshape(N_BLK, N_AUX)
    pairs_grid = pair_list.reshape(N_BLK, PAIRS_DEV, 2)
    ranks_grid = pair_ranks.reshape(N_BLK, PAIRS_DEV)
    amps_grid = amplitudes.reshape(N_BLK, PAIRS_DEV, R, R)

    def owner_sum(owner_index):
        accum = jnp.zeros((PAIRS_DEV, R, R), jnp.float32)
        for offset in range(3):
            source = (owner_index - offset) % N_BLK
            for member in range(N_AUX):
                accum = accum + ladder(blocked[:, source, member], counts_grid[source, member], pairs_grid[owner_index], ranks_grid[owner_index], amps_grid[owner_index])
        return accum

    result = lax.map(owner_sum, jnp.arange(N_BLK, dtype=jnp.int32))
    return result.reshape(N_BLK * PAIRS_DEV, R, R)
```

```python
import functools

import jax
import jax.numpy as jnp
from jax import lax
from jax.experimental import pallas as pl
from jax.experimental.pallas import tpu as pltpu
from jax.sharding import PartitionSpec as P

LANES = 128
HALF_LANES = 64
ROW_CLASSES = (64, 96, 112, 128)


def passed_along(value, axis, steps):
    count = lax.axis_size(axis)
    pairs = [(source, (source + steps) % count) for source in range(count)]
    return lax.ppermute(value, axis, pairs)


MOST = 176
COUNT = 2


def block_sizes(slots):
    largest = 4
    for size in range(4, min(slots, MOST) + 1, 4):
        if slots % size == 0:
            largest = size
    sizes = [largest]
    while len(sizes) < COUNT and sizes[-1] % 8 == 0:
        sizes.append(sizes[-1] // 2)
    return sizes


def ladder_kernel(
    sizes, per_owner, first_owner, owners, splits,
    place, counts, pairs, ranks, amps, panels, out, held, weights, ready, arrived,
):
    orbitals, slots, width, _ = panels.shape
    pair_total = amps.shape[0]
    big, piece = sizes[0], sizes[-1]
    parts = big // piece
    rounds = slots // big
    count = counts[place[0] * splits + place[1]]
    live_pieces = (count + piece - 1) // piece

    def row_of(pair):
        owner = lax.rem(place[0] + first_owner + pair // per_owner, owners)
        return owner * per_owner + lax.rem(pair, per_owner)

    def transfer(orbital, index):
        span = pl.ds(index * piece, piece)
        return pltpu.make_async_copy(
            panels.at[orbital, span], held.at[orbital, span], arrived.at[orbital, index]
        )

    def start_orbital(orbital, turn):
        ready[orbital, turn] = 1
        for part in range(parts):
            index = turn * parts + part

            @pl.when(index < live_pieces)
            def _():
                transfer(orbital, index).start()

    def finish_orbital(orbital, turn):
        @pl.when(ready[orbital, turn] == 1)
        def _():
            ready[orbital, turn] = 2
            for part in range(parts):
                index = turn * parts + part

                @pl.when(index < live_pieces)
                def _():
                    transfer(orbital, index).wait()

    for turn in range(rounds):
        for orbital in range(orbitals):
            ready[orbital, turn] = 0
    for turn in range(rounds):
        def start_pair(pair, carry):
            for side in range(2):
                orbital = pairs[2 * row_of(pair) + side]

                @pl.when(ready[orbital, turn] == 0)
                def _():
                    start_orbital(orbital, turn)
            return carry

        lax.fori_loop(0, pair_total, start_pair, 0)

    def prepare(pair, carry):
        rank = ranks[row_of(pair)]
        value = amps[pair]
        row = lax.broadcasted_iota(jnp.int32, value.shape, 0)
        lane = lax.broadcasted_iota(jnp.int32, value.shape, 1)
        value = jnp.where((row < rank) & (lane < rank), value, jnp.zeros_like(value))
        weights[pair] = jnp.zeros(weights.shape[1:], weights.dtype)
        out[pair] = jnp.zeros(out.shape[1:], out.dtype)

        @pl.when(rank <= HALF_LANES)
        def _():
            small = value[:HALF_LANES, :HALF_LANES]
            for spot in range(0, 2 * LANES, HALF_LANES):
                weights[pair, spot:spot + HALF_LANES, spot:spot + HALF_LANES] = small

        @pl.when(rank > HALF_LANES)
        def _():
            for spot in range(0, 2 * LANES, LANES):
                weights[pair, spot:spot + width, spot:spot + width] = value

        return carry

    lax.fori_loop(0, pair_total, prepare, 0)

    def slab(orbital, slot, rows, bound):
        kept = min(rows, width)
        value = held[orbital, slot, :kept, :]
        if bound is not None:
            value = jnp.where(slot < bound, value, jnp.zeros_like(value))
        if rows == HALF_LANES:
            return value[:, :HALF_LANES]
        value = jnp.concatenate([value, jnp.zeros((kept, LANES - width), value.dtype)], 1)
        if rows > kept:
            value = jnp.concatenate([value, jnp.zeros((rows - kept, LANES), value.dtype)], 0)
        return value

    def block(pair, left, right, base, size, rows):
        group = 4 if rows == HALF_LANES else 2

        def joined(orbital, index, bound):
            return jnp.concatenate(
                [slab(orbital, base + index * group + part, rows, bound) for part in range(group)], 1
            )

        steps = size // group
        lhs = jnp.concatenate([joined(left, index, count) for index in range(steps)], 0)
        half = jnp.dot(lhs, weights[pair], preferred_element_type=jnp.float32).astype(jnp.bfloat16)
        total = None
        for index in range(steps):
            term = lax.dot_general(
                half[index * rows:(index + 1) * rows], joined(right, index, None),
                (((1,), (1,)), ((), ())), preferred_element_type=jnp.float32,
            )
            total = term if total is None else total + term
        kept = min(rows, width)
        out[pair, :kept, :kept] += total[:kept, :kept]

    def one_round(turn, carry):
        base = turn * big
        amount = jnp.clip((count - base + piece - 1) // piece, 0, parts)

        def one_pair(pair, carry):
            place_of = row_of(pair)
            left, right = pairs[2 * place_of], pairs[2 * place_of + 1]
            rank = ranks[place_of]
            finish_orbital(left, turn)
            finish_orbital(right, turn)

            def arm(rows):
                def run():
                    for size in sizes:
                        share = size // piece
                        if size == big:
                            wanted, offset = amount == share, 0
                        else:
                            wanted = ((amount // share) % 2 == 1) & (amount < parts)
                            offset = amount // (2 * share) * (2 * share) * piece
                        pl.when(wanted)(functools.partial(block, pair, left, right, base + offset, size, rows))
                return run

            choice = sum((rank > rows).astype(jnp.int32) for rows in ROW_CLASSES[:-1])
            lax.switch(choice, [arm(rows) for rows in ROW_CLASSES])
            return carry

        return lax.fori_loop(0, pair_total, one_pair, carry)

    lax.fori_loop(0, rounds, one_round, 0)

    def trim(pair, carry):
        rank = ranks[row_of(pair)]
        value = out[pair]
        row = lax.broadcasted_iota(jnp.int32, value.shape, 0)
        lane = lax.broadcasted_iota(jnp.int32, value.shape, 1)
        out[pair] = jnp.where((row < rank) & (lane < rank), value, jnp.zeros_like(value))
        return carry

    lax.fori_loop(0, pair_total, trim, 0)


def ladder(place, counts, pairs, ranks, amps, panels, per_owner, first_owner, owners, splits):
    orbitals, slots, width, _ = panels.shape
    pair_total = amps.shape[0]
    sizes = block_sizes(slots)
    flops = 2 * pair_total * slots * LANES * LANES * LANES
    return pl.pallas_call(
        functools.partial(ladder_kernel, sizes, per_owner, first_owner, owners, splits),
        out_shape=jax.ShapeDtypeStruct((pair_total, width, width), jnp.float32),
        grid_spec=pltpu.PrefetchScalarGridSpec(
            num_scalar_prefetch=4,
            grid=(1,),
            in_specs=[
                pl.BlockSpec((pair_total, width, width), lambda *_: (0, 0, 0)),
                pl.BlockSpec(memory_space=pl.ANY),
            ],
            out_specs=pl.BlockSpec((pair_total, width, width), lambda *_: (0, 0, 0)),
            scratch_shapes=[
                pltpu.VMEM((orbitals, slots, width, width), panels.dtype),
                pltpu.VMEM((pair_total, 2 * LANES, 2 * LANES), jnp.bfloat16),
                pltpu.SMEM((orbitals, slots // sizes[0]), jnp.int32),
                pltpu.SemaphoreType.DMA((orbitals, slots // sizes[-1])),
            ],
        ),
        compiler_params=pltpu.CompilerParams(
            dimension_semantics=("arbitrary",), vmem_limit_bytes=60 * 1024 * 1024
        ),
        cost_estimate=pl.CostEstimate(flops=flops, bytes_accessed=2 * panels.size, transcendentals=0),
    )(place, counts, pairs.reshape(-1), ranks, amps, panels)


def shards(panels, aux_counts, pair_list, pair_ranks, amplitudes):
    owners, splits = lax.axis_size("blk"), lax.axis_size("aux")
    per_owner, width = amplitudes.shape[:2]
    place = jnp.stack([lax.axis_index("blk"), lax.axis_index("aux")]).astype(jnp.int32)
    run = functools.partial(
        ladder, place, aux_counts, pair_list, pair_ranks,
        panels=panels, per_owner=per_owner, owners=owners, splits=splits,
    )
    others = jnp.concatenate(
        [passed_along(amplitudes, "blk", -1), passed_along(amplitudes, "blk", -2)], 0
    )
    away = run(amps=others, first_owner=1)
    near = passed_along(away[:per_owner], "blk", 1)
    far = passed_along(away[per_owner:], "blk", 2)
    home = run(amps=amplitudes, first_owner=0)
    total = home + near + far
    share = width // splits
    mine = lax.axis_index("aux")
    parts = total.reshape(per_owner, splits, share, width)
    result = lax.dynamic_index_in_dim(parts, mine, 1, keepdims=False)
    for step in range(1, splits):
        gone = lax.dynamic_index_in_dim(parts, (mine + step) % splits, 1, keepdims=False)
        result = result + passed_along(gone, "aux", step)
    return result


def solution(mesh):
    placed = (P(None, ("blk", "aux"), None, None), P(), P(), P(), P("blk", None, None))
    return jax.shard_map(
        shards, mesh=mesh, in_specs=placed, out_specs=P("blk", "aux", None), check_vma=False
    )
```

```python
import functools

import jax
import jax.numpy as jnp
from jax import lax
from jax.experimental import pallas as pl
from jax.experimental.pallas import tpu as pltpu
from jax.sharding import PartitionSpec as P

LANES = 128
HALF_LANES = 64
LONG_CLASSES = (48, 64, 80, 96, 112, 128)
SHORT_CLASSES = (64, 96, 128)


def passed_along(value, axis, steps):
    count = lax.axis_size(axis)
    pairs = [(source, (source + steps) % count) for source in range(count)]
    return lax.ppermute(value, axis, pairs)


MOST = 176
COUNT = 2


def block_sizes(slots):
    largest = 4
    for size in range(4, min(slots, MOST) + 1, 4):
        if slots % size == 0:
            largest = size
    sizes = [largest]
    while len(sizes) < COUNT and sizes[-1] % 8 == 0:
        sizes.append(sizes[-1] // 2)
    return sizes


def ladder_kernel(
    sizes, per_owner, first_owner, owners, splits,
    place, counts, pairs, ranks, *refs,
):
    held, sums, weights, ready, arrived = refs[-5:]
    groups = (len(refs) - 6) // 2
    amps, panels, outs = refs[:groups], refs[groups], refs[groups + 1:2 * groups + 1]
    orbitals, slots, width, _ = panels.shape
    pair_total = per_owner * len(amps)
    big, piece = sizes[0], sizes[-1]
    parts = big // piece
    rounds = slots // big
    count = counts[place[0] * splits + place[1]]
    live_pieces = (count + piece - 1) // piece

    def row_of(pair):
        owner = lax.rem(place[0] + first_owner + pair // per_owner, owners)
        return owner * per_owner + lax.rem(pair, per_owner)

    def transfer(orbital, index):
        span = pl.ds(index * piece, piece)
        return pltpu.make_async_copy(
            panels.at[orbital, span], held.at[orbital, span], arrived.at[orbital, index]
        )

    def start(orbital, index):
        @pl.when((index < live_pieces) & (ready[orbital, index] == 0))
        def _():
            ready[orbital, index] = 1
            transfer(orbital, index).start()

    def finish(orbital, index):
        @pl.when(ready[orbital, index] == 1)
        def _():
            ready[orbital, index] = 2
            transfer(orbital, index).wait()

    for orbital in range(orbitals):
        for index in range(rounds * parts):
            ready[orbital, index] = 0
    for turn in range(rounds):
        def start_pair(pair, carry):
            for part in range(parts):
                for side in range(2):
                    start(pairs[2 * row_of(pair) + side], turn * parts + part)
            return carry

        lax.fori_loop(0, pair_total, start_pair, 0)

    def inside(value, rank):
        row = lax.broadcasted_iota(jnp.int32, value.shape, 0)
        lane = lax.broadcasted_iota(jnp.int32, value.shape, 1)
        return jnp.where((row < rank) & (lane < rank), value, jnp.zeros_like(value))

    for group in range(groups):
        def prepare(spot_of, carry):
            pair = group * per_owner + spot_of
            rank = ranks[row_of(pair)]
            value = inside(amps[group][spot_of], rank)
            weights[pair] = jnp.zeros(weights.shape[1:], weights.dtype)
            sums[pair] = jnp.zeros(sums.shape[1:], sums.dtype)

            @pl.when(rank <= HALF_LANES)
            def _():
                small = value[:HALF_LANES, :HALF_LANES]
                for spot in range(0, 2 * LANES, HALF_LANES):
                    weights[pair, spot:spot + HALF_LANES, spot:spot + HALF_LANES] = small

            @pl.when(rank > HALF_LANES)
            def _():
                for spot in range(0, 2 * LANES, LANES):
                    weights[pair, spot:spot + width, spot:spot + width] = value

            return carry

        lax.fori_loop(0, per_owner, prepare, 0)

    def slab(orbital, slot, rows, bound):
        kept = min(rows, width)
        value = held[orbital, slot, :kept, :]
        if bound is not None:
            value = jnp.where(slot < bound, value, jnp.zeros_like(value))
        if rows <= HALF_LANES:
            return value[:, :HALF_LANES]
        value = jnp.concatenate([value, jnp.zeros((kept, LANES - width), value.dtype)], 1)
        if rows > kept:
            value = jnp.concatenate([value, jnp.zeros((rows - kept, LANES), value.dtype)], 0)
        return value

    def block(pair, left, right, base, size, rows):
        group = 4 if rows <= HALF_LANES else 2

        def joined(orbital, index, bound):
            return jnp.concatenate(
                [slab(orbital, base + index * group + part, rows, bound) for part in range(group)], 1
            )

        steps = size // group
        lhs = jnp.concatenate([joined(left, index, count) for index in range(steps)], 0)
        half = jnp.dot(lhs, weights[pair], preferred_element_type=jnp.float32).astype(jnp.bfloat16)
        total = None
        for index in range(steps):
            term = lax.dot_general(
                half[index * rows:(index + 1) * rows], joined(right, index, None),
                (((1,), (1,)), ((), ())), preferred_element_type=jnp.float32,
            )
            total = term if total is None else total + term
        kept = min(rows, width)
        sums[pair, :kept, :kept] += total[:kept, :kept]

    def one_round(turn, carry):
        base = turn * big
        amount = jnp.clip((count - base + piece - 1) // piece, 0, parts)

        def one_pair(pair, carry):
            place_of = row_of(pair)
            left, right = pairs[2 * place_of], pairs[2 * place_of + 1]
            rank = ranks[place_of]

            def run(base, size, classes):
                choice = sum((rank > rows).astype(jnp.int32) for rows in classes[:-1])
                lax.switch(choice, [
                    functools.partial(block, pair, left, right, base, size, rows) for rows in classes
                ])

            whole = amount == parts
            if parts > 1:
                whole = whole & ((turn > 0) | (pair > 0))

                def one_piece(part, carry):
                    finish(left, turn * parts + part)
                    finish(right, turn * parts + part)
                    run(base + part * piece, piece, SHORT_CLASSES)
                    return carry

                lax.fori_loop(0, jnp.where(whole, 0, amount), one_piece, 0)

            @pl.when(whole)
            def _():
                for part in range(parts):
                    finish(left, turn * parts + part)
                    finish(right, turn * parts + part)
                run(base, big, LONG_CLASSES)

            return carry

        return lax.fori_loop(0, pair_total, one_pair, carry)

    lax.fori_loop(0, rounds, one_round, 0)

    for group in range(groups):
        def trim(spot_of, carry):
            pair = group * per_owner + spot_of
            outs[group][spot_of] = inside(sums[pair], ranks[row_of(pair)])
            return carry

        lax.fori_loop(0, per_owner, trim, 0)


def ladder(place, counts, pairs, ranks, amps, panels, first_owner, owners, splits):
    orbitals, slots, width, _ = panels.shape
    per_owner = amps[0].shape[0]
    pair_total = per_owner * len(amps)
    sizes = block_sizes(slots)
    flops = 2 * pair_total * slots * LANES * LANES * LANES
    whole = pl.BlockSpec((per_owner, width, width), lambda *_: (0, 0, 0))
    return pl.pallas_call(
        functools.partial(ladder_kernel, sizes, per_owner, first_owner, owners, splits),
        out_shape=[jax.ShapeDtypeStruct((per_owner, width, width), jnp.float32) for _ in amps],
        grid_spec=pltpu.PrefetchScalarGridSpec(
            num_scalar_prefetch=4,
            grid=(1,),
            in_specs=[whole for _ in amps] + [pl.BlockSpec(memory_space=pl.ANY)],
            out_specs=[whole for _ in amps],
            scratch_shapes=[
                pltpu.VMEM((orbitals, slots, width, width), panels.dtype),
                pltpu.VMEM((pair_total, width, width), jnp.float32),
                pltpu.VMEM((pair_total, 2 * LANES, 2 * LANES), jnp.bfloat16),
                pltpu.SMEM((orbitals, slots // sizes[-1]), jnp.int32),
                pltpu.SemaphoreType.DMA((orbitals, slots // sizes[-1])),
            ],
        ),
        compiler_params=pltpu.CompilerParams(
            dimension_semantics=("arbitrary",), vmem_limit_bytes=60 * 1024 * 1024
        ),
        cost_estimate=pl.CostEstimate(flops=flops, bytes_accessed=2 * panels.size, transcendentals=0),
    )(place, counts, pairs.reshape(-1), ranks, *amps, panels)


def shards(panels, aux_counts, pair_list, pair_ranks, amplitudes):
    owners, splits = lax.axis_size("blk"), lax.axis_size("aux")
    per_owner, width = amplitudes.shape[:2]
    place = jnp.stack([lax.axis_index("blk"), lax.axis_index("aux")]).astype(jnp.int32)
    run = functools.partial(
        ladder, place, aux_counts, pair_list, pair_ranks, panels=panels, owners=owners, splits=splits
    )
    away = run(
        amps=[passed_along(amplitudes, "blk", -1), passed_along(amplitudes, "blk", -2)], first_owner=1
    )
    near, far = passed_along(away[0], "blk", 1), passed_along(away[1], "blk", 2)
    (home,) = run(amps=[amplitudes], first_owner=0)
    total = home + near + far
    share = width // splits
    mine = lax.axis_index("aux")
    parts = total.reshape(per_owner, splits, share, width)
    result = lax.dynamic_index_in_dim(parts, mine, 1, keepdims=False)
    for step in range(1, splits):
        gone = lax.dynamic_index_in_dim(parts, (mine + step) % splits, 1, keepdims=False)
        result = result + passed_along(gone, "aux", step)
    return result


def solution(mesh):
    placed = (P(None, ("blk", "aux"), None, None), P(), P(), P(), P("blk", None, None))
    return jax.shard_map(
        shards, mesh=mesh, in_specs=placed, out_specs=P("blk", "aux", None), check_vma=False
    )
```
